32 devices in a mesh: region: 4 (over y, x), blk: 8 (over z, core).
Axes of the slice: x: 2, y: 2, z: 4, core: 2. Of those that a mesh axis runs over, the one named last changes fastest.
Arguments:
- incident: bfloat16 [8, 4, 64, 32, 128], P(None, 'region', 'blk'), may hold values from -6 to 6
- past_currents: bfloat16 [4, 4, 64, 32, 128], P(None, 'region', 'blk'), may hold values from -6 to 6
- self_inverse: bfloat16 [4, 64, 128, 128], P('region', 'blk'), may hold values from -0.5 to 0.5
- near_tiles: bfloat16 [4, 64, 32, 128, 128], P('region', 'blk'), may hold values from -0.046875 to 0.046875
- near_cols: int32 [4, 64, 32], P('region', 'blk'), may hold values from 0 to 63, as said below
- near_delay: int32 [4, 64, 32], P('region', 'blk'), may hold values from 1 to 4
- block_slot: int32 [4, 64], P('region'), may hold values from 0 to 63, as said below
- far_out: bfloat16 [4, 64, 128, 64], P('region', 'blk'), may hold values from -0.03125 to 0.03125
- far_in: bfloat16 [4, 64, 64, 128], P('region', 'blk'), may hold values from -0.75 to 0.75
- far_pairs: int32 [4, 3], P('region'), may hold values from 0 to 3, as said below
- far_delay: int32 [4, 3], P('region'), may hold values from 1 to 4
- far_coupling: float32 [4, 3, 64, 64], P('region'), may hold values from -0.4375 to 0.4375
Outputs:
- currents: bfloat16 [8, 4, 64, 32, 128], P(None, 'region', 'blk')
The draws below stay inside these ranges and needn't reach their ends.
Inputs may be any that keep to these rules, and one draw needn't show every extreme that they name: `block_slot`: each region's ids are a permutation of 0 to 63. `near_cols`: for block row at position b, every near source block is stored on a blk device at most 4 devices from the device of b, and the first tile of every row lies exactly 4 devices away. `far_pairs`: region g lists each of the other 3 regions exactly once.
All inputs are finite; a program needn't handle non-finite values.
Results may differ from the reference program's by a relative error of at most 0.01.
Values may be sent and summed in bfloat16 or wider, within the bound.
A program may use at most 64 MiB of HBM per device.

```python
import jax
import jax.numpy as jnp
from jax import lax

ROWS = 128
PULSES = 32
RANK = 64
BLK_DEV = 8
NEAR = 32
STEPS = 8
DMAX = 4
REACH = 4
REGIONS = 4
GB = 64
FARP = 3


def layout(key):
    base = jax.random.fold_in(key, 7)
    keys = jax.random.split(base, 3)
    slots = jax.vmap(lambda inner: jax.random.permutation(inner, GB))(jax.random.split(keys[0], REGIONS)).astype(jnp.int32)
    devices = GB // BLK_DEV
    home = (jnp.arange(GB, dtype=jnp.int32) // BLK_DEV)[None, :, None]
    offsets = jax.random.randint(keys[1], (REGIONS, GB, NEAR), -REACH, REACH + 1)
    edge = jnp.where(home + REACH < devices, REACH, -REACH)
    offsets = jnp.concatenate([jnp.broadcast_to(edge, (REGIONS, GB, 1)), offsets[:, :, 1:]], axis=2)
    target_dev = jnp.clip(home + offsets, 0, devices - 1)
    within = jax.random.randint(keys[2], (REGIONS, GB, NEAR), 0, BLK_DEV)
    target = (target_dev * BLK_DEV + within).astype(jnp.int32)
    inverse = jnp.argsort(slots, axis=1, stable=True).astype(jnp.int32)
    ids = jnp.take_along_axis(inverse, target.reshape(REGIONS, -1), axis=1).reshape(REGIONS, GB, NEAR)
    return (slots, ids.astype(jnp.int32))


def draw_block_slot(key, part):
    return layout(key)[0]


def draw_near_cols(key, part):
    return layout(key)[1]


def draw_far_pairs(key, part):
    base = jax.random.fold_in(key, 13)
    others = jax.vmap(lambda inner: jax.random.permutation(inner, REGIONS - 1))(jax.random.split(base, REGIONS)).astype(jnp.int32)
    owner = jnp.arange(REGIONS, dtype=jnp.int32)[:, None]
    return (others + (others >= owner).astype(jnp.int32)).astype(jnp.int32)


def set_ends(array, rng, low, largest):
    spot = [jax.random.randint(jax.random.fold_in(rng, axis), (), 0, length) for axis, length in enumerate(array.shape)]
    longest = array.shape.index(max(array.shape))
    beside = spot[:longest] + [(spot[longest] + 1) % array.shape[longest]] + spot[longest + 1:]
    return array.at[tuple(spot)].set(low).at[tuple(beside)].set(largest)


def level_of(rng, extent, shards, smallest, top_value):
    def one(axis_at, parts):
        steps = jax.random.uniform(jax.random.fold_in(jax.random.fold_in(rng, 6), axis_at), (parts,), jnp.float32, smallest / len(shards), top_value / len(shards))
        return jnp.repeat(jnp.exp(steps), extent[axis_at] // parts).reshape((-1,) + (1,) * (len(extent) - axis_at - 1))

    level = one(*shards[0])
    for cut in shards[1:]:
        level = level * one(*cut)
    return level


def normal_values(own_key, dims, spread, most, cuts=(), held_as=jnp.bfloat16):
    factor_of = level_of(own_key, dims, cuts, -0.22, 0.18) if cuts else 1.0
    entries = jax.random.normal(own_key, dims, jnp.float32) * spread * factor_of
    return jnp.minimum(jnp.maximum(entries, -most), most).astype(held_as)


def setup_inputs(seed: int = 0) -> dict:
    arg_keys = jax.random.split(jax.random.key(seed), 13)
    return {
        "incident": normal_values(arg_keys[0], (STEPS, REGIONS, GB, PULSES, ROWS), 1.0, 6.0, ((1, 4), (2, 8))),
        "past_currents": normal_values(arg_keys[1], (DMAX, REGIONS, GB, PULSES, ROWS), 1.0, 6.0, ((1, 4), (2, 8))),
        "self_inverse": normal_values(arg_keys[2], (REGIONS, GB, ROWS, ROWS), ROWS ** -0.5, 0.5, ((0, 4), (1, 8))),
        "near_tiles": normal_values(arg_keys[3], (REGIONS, GB, NEAR, ROWS, ROWS), (4 * ROWS * NEAR) ** -0.5, 0.046875, ((0, 4), (1, 8))),
        "near_cols": draw_near_cols(jax.random.fold_in(arg_keys[12], 71), 0),
        "near_delay": set_ends(jax.random.randint(arg_keys[5], (REGIONS, GB, NEAR), 1, DMAX + 1), jax.random.fold_in(arg_keys[5], 1), 1, DMAX).astype(jnp.int32),
        "block_slot": draw_block_slot(jax.random.fold_in(arg_keys[12], 71), 0),
        "far_out": normal_values(arg_keys[7], (REGIONS, GB, ROWS, RANK), (4 * ROWS * GB) ** -0.5, 0.03125, ((0, 4), (1, 8))),
        "far_in": normal_values(arg_keys[8], (REGIONS, GB, RANK, ROWS), RANK ** -0.5, 0.75, ((0, 4), (1, 8))),
        "far_pairs": draw_far_pairs(jax.random.fold_in(arg_keys[12], 71), 0),
        "far_delay": set_ends(jax.random.randint(arg_keys[10], (REGIONS, FARP), 1, DMAX + 1), jax.random.fold_in(arg_keys[10], 1), 1, DMAX).astype(jnp.int32),
        "far_coupling": normal_values(arg_keys[11], (REGIONS, FARP, RANK, RANK), (RANK * FARP) ** -0.5, 0.4375, ((0, 4),), jnp.float32),
    }


def moments(current, far_out):
    return jnp.einsum('gbpr,gbrk->gpk', current.astype(jnp.float32), far_out.astype(jnp.float32))


def near_region(packed):
    history, tiles, position, delays = packed
    sources = history[delays - 1, position]
    return jnp.einsum('bjpk,bjkm->bpm', sources.astype(jnp.float32), tiles.astype(jnp.float32))


def reference(incident, past_currents, self_inverse, near_tiles, near_cols, near_delay, block_slot, far_out, far_in, far_pairs, far_delay, far_coupling):
    regions = block_slot.shape[0]
    position = jnp.take_along_axis(block_slot, near_cols.reshape(regions, -1), axis=1).reshape(near_cols.shape).astype(jnp.int32)
    history = past_currents
    moment_hist = jnp.stack([moments(past_currents[k], far_out) for k in range(DMAX)])
    outputs = []
    for step in range(STEPS):
        sources = moment_hist[far_delay - 1, far_pairs]
        blended = jnp.einsum('gfpk,gfkl->gpl', sources, far_coupling, precision=lax.Precision.HIGHEST).astype(jnp.bfloat16)
        far_field = jnp.einsum('gpk,gbkr->gbpr', blended.astype(jnp.float32), far_in.astype(jnp.float32))
        near_field = lax.map(near_region, (jnp.moveaxis(history, 1, 0), near_tiles, position, near_delay))
        driven = (incident[step].astype(jnp.float32) - near_field - far_field).astype(jnp.bfloat16)
        current = jnp.einsum('gbpk,gbkm->gbpm', driven.astype(jnp.float32), self_inverse.astype(jnp.float32)).astype(jnp.bfloat16)
        outputs.append(current)
        history = jnp.concatenate([current[None], history[:-1]], axis=0)
        moment_hist = jnp.concatenate([moments(current, far_out)[None], moment_hist[:-1]], axis=0)
    return jnp.stack(outputs)
```

```python
import functools

import jax
import jax.numpy as jnp
from jax import lax
from jax.experimental import pallas as pl
from jax.experimental.pallas import tpu as pltpu
from jax.sharding import PartitionSpec as P

REACH = 4
CORES = 2
HOPS = (REACH + CORES - 1) // CORES
WIN = CORES * (2 * HOPS + 1)
F32 = jnp.float32
BF16 = jnp.bfloat16
MESH = pl.DeviceIdType.MESH


def march(
    regions, devices, chunks,
    cols_ref, delay_ref, slot_ref, pairs_ref, fdelay_ref,
    inc_hbm, past_hbm, sinv_hbm, tiles_hbm, fout_hbm, fin_hbm, cpl_hbm,
    out_ref,
    win, hist, tiles, inc, sinv, fout, fin, fin2, cpl, cpl2,
    msend, mrecv, msum, bsend, brecv, bl2, pos,
    in_sem, past_sem, tile_sem,
    own_send, fwd_send, own_recv, past_send, pastf_send, past_recv,
    m_send, m_recv, mp_send, mp_recv, b_send, b_recv,
):
    steps = inc_hbm.shape[0]
    dmax = past_hbm.shape[0]
    nb, near = tiles.shape[0], tiles.shape[1]
    per = nb // chunks
    pulses, rows = inc.shape[2], inc.shape[3]
    half, rank = pulses // 2, fout.shape[2]
    farp = cpl.shape[0]
    places = devices // CORES
    g = lax.axis_index("region")
    d = lax.axis_index("blk")
    z = d // CORES
    c = d % CORES
    mate = CORES * z + (1 - c)
    own = CORES * HOPS + c
    has_dn = d >= CORES
    has_up = d + CORES < devices

    past_in = [
        pltpu.make_async_copy(past_hbm.at[k, 0], win.at[dmax - 1 - k, own], past_sem.at[k])
        for k in range(dmax)
    ]
    small_in = [
        pltpu.make_async_copy(fout_hbm.at[0], fout, in_sem.at[0]),
        pltpu.make_async_copy(fin_hbm.at[0], fin, in_sem.at[1]),
        pltpu.make_async_copy(cpl_hbm.at[0], cpl, in_sem.at[2]),
        pltpu.make_async_copy(sinv_hbm.at[0], sinv, in_sem.at[3]),
        pltpu.make_async_copy(inc_hbm.at[:, 0], inc, in_sem.at[4]),
    ]
    tile_in = [
        pltpu.make_async_copy(tiles_hbm.at[0, b], tiles.at[b], tile_sem.at[b]) for b in range(nb)
    ]
    for copy in past_in + small_in + tile_in:
        copy.start()

    barrier = pltpu.get_barrier_semaphore()

    def greet(region, blk):
        pl.semaphore_signal(barrier, inc=1, device_id=(region, blk), device_id_type=MESH)

    greet(g, mate)

    @pl.when(has_dn)
    def _():
        greet(g, d - CORES)

    @pl.when(has_up)
    def _():
        greet(g, d + CORES)

    others = [(g + r) % regions for r in range(1, regions)]
    for g2 in others:
        for z2 in range(places):
            greet(g2, CORES * z2 + c)

    ends = has_dn.astype(jnp.int32) + has_up.astype(jnp.int32)
    pl.semaphore_wait(barrier, 1 + ends + (regions - 1) * places)

    def part(t, slot, ch, size):
        return win.at[t, slot, pl.ds(ch * size, size)]

    def send(t, ch, size, slot, slot2, dev, ssem, rsem):
        return pltpu.make_async_remote_copy(
            src_ref=part(t, slot, ch, size),
            dst_ref=part(t, slot2, ch, size),
            send_sem=ssem,
            recv_sem=rsem,
            device_id=(g, dev),
            device_id_type=MESH,
        )

    def own_copies(t, ch, size, ssem, rsem):
        return [
            (has_dn, send(t, ch, size, own, own + CORES, d - CORES, ssem.at[0], rsem.at[own + CORES])),
            (has_up, send(t, ch, size, own, own - CORES, d + CORES, ssem.at[1], rsem.at[own - CORES])),
            (None, send(t, ch, size, own, own, mate, ssem.at[2], rsem.at[own])),
        ]

    def arrivals(t, ch, size, hop, fsem, rsem):
        found = []
        for side, sign in enumerate((-1, 1)):
            source = d + sign * CORES * hop
            present = (source >= 0) & (source < devices)
            slot = own + sign * CORES * hop
            onward = d - sign * CORES
            more = present & (onward >= 0) & (onward < devices) if hop < HOPS else None
            forward = None
            if hop < HOPS:
                forward = send(
                    t, ch, size, slot, slot + sign * CORES, onward,
                    fsem.at[hop - 1, side, 0], rsem.at[slot + sign * CORES],
                )
            relay = send(t, ch, size, slot, slot, mate, fsem.at[hop - 1, side, 1], rsem.at[slot])
            found.append((present, slot, more, forward, relay))
        return found

    def guarded(cond, run):
        if cond is None:
            run()
        else:
            pl.when(cond)(run)

    def start(copies):
        for cond, copy in copies:
            guarded(cond, copy.start)

    def landed(t, ch, size, slot, rsem):
        ref = part(t, slot, ch, size)
        pltpu.make_async_copy(ref, ref, rsem.at[slot]).wait()

    def pass_on(t, ch, size, hop, fsem, rsem):
        for present, slot, more, forward, relay in arrivals(t, ch, size, hop, fsem, rsem):
            @pl.when(present)
            def _(slot=slot, relay=relay):
                landed(t, ch, size, slot, rsem)

            if forward is not None:
                pl.when(more)(forward.start)

            pl.when(present)(relay.start)

    def from_mate(t, ch, size, rsem):
        for hop in range(-HOPS, HOPS + 1):
            slot = CORES * HOPS + (1 - c) + CORES * hop
            source = mate + CORES * hop

            def take(slot=slot):
                landed(t, ch, size, slot, rsem)

            guarded(None if hop == 0 else (source >= 0) & (source < devices), take)

    def sent(t, ch, size, ssem, fsem, rsem):
        for cond, copy in own_copies(t, ch, size, ssem, rsem):
            guarded(cond, copy.wait_send)
        for hop in range(1, HOPS + 1):
            for present, slot, more, forward, relay in arrivals(t, ch, size, hop, fsem, rsem):
                if forward is not None:
                    pl.when(more)(forward.wait_send)
                pl.when(present)(relay.wait_send)

    def keep(t, ring):
        for k in range(WIN):
            source = CORES * (z - HOPS) + k

            @pl.when((source >= 0) & (source < devices))
            def _(k=k):
                hist[pl.ds((ring * WIN + k) * nb, nb)] = win[t, k]

    def pack(moment):
        return jnp.concatenate([moment[:half], moment[half:]], axis=1)

    def moment_copies(t, source, ssem, rsem):
        copies = []
        for r, g2 in enumerate(others):
            for z2 in range(places):
                copies.append(
                    pltpu.make_async_remote_copy(
                        src_ref=source,
                        dst_ref=mrecv.at[t, g, z],
                        send_sem=ssem.at[r, z2],
                        recv_sem=rsem.at[g, z],
                        device_id=(g2, CORES * z2 + c),
                        device_id_type=MESH,
                    )
                )
        return copies

    def take_moments(t, ring, rsem):
        for g2 in others:
            total = None
            for z2 in range(places):
                ref = mrecv.at[t, g2, z2]
                pltpu.make_async_copy(ref, ref, rsem.at[g2, z2]).wait()
            for z2 in range(places):
                value = mrecv[t, g2, z2].astype(F32)
                total = value if total is None else total + value
            msum[ring, g2] = total

    def blend(n, parity):
        total = None
        for p in range(farp):
            ring = lax.rem(n + dmax - fdelay_ref[0, p], dmax)
            value = jnp.dot(
                msum[ring, pairs_ref[0, p]], cpl2[p],
                preferred_element_type=F32, precision=lax.Precision.HIGHEST,
            )
            total = value if total is None else total + value
        bsend[...] = total
        copy = pltpu.make_async_remote_copy(
            src_ref=bsend, dst_ref=brecv.at[parity], send_sem=b_send, recv_sem=b_recv.at[parity],
            device_id=(g, mate), device_id_type=MESH,
        )
        copy.start()
        copy.wait()
        both = (total + brecv[parity]).astype(BF16)
        lane = lax.broadcasted_iota(jnp.int32, both.shape, 1)
        zero = jnp.zeros_like(both)
        bl2[...] = jnp.concatenate(
            [jnp.where(lane < rank, both, zero), jnp.where(lane < rank, zero, both)], axis=0
        )

    for k in range(dmax):
        past_in[k].wait()
    for t in range(dmax):
        start(own_copies(t, 0, nb, past_send.at[t], past_recv.at[t]))
    small_in[0].wait()
    for t in range(dmax):
        moment = None
        for b in range(nb):
            value = jnp.dot(win[t, own, b], fout[b], preferred_element_type=F32)
            moment = value if moment is None else moment + value
        msend[t] = pack(moment).astype(BF16)
    for t in range(dmax):
        for copy in moment_copies(t, msend.at[t], mp_send.at[t], mp_recv.at[t]):
            copy.start()

    def place(i, carry):
        b, j = i // near, i % near
        where = slot_ref[0, cols_ref[0, b, j]] - CORES * (z - HOPS) * nb
        pos[i] = jnp.minimum(jnp.maximum(where, 0), WIN * nb - 1)
        return carry

    lax.fori_loop(0, nb * near, place, 0)
    small_in[1].wait()
    small_in[2].wait()
    for b in range(nb):
        fin2[b, :rank] = fin[b]
        fin2[b, rank:] = fin[b]
    for p in range(farp):
        value = cpl[p]
        blank = jnp.zeros_like(value)
        cpl2[p, :rank] = jnp.concatenate([value, blank], axis=1)
        cpl2[p, rank:] = jnp.concatenate([blank, value], axis=1)

    for hop in range(1, HOPS + 1):
        for t in range(dmax):
            pass_on(t, 0, nb, hop, pastf_send.at[t], past_recv.at[t])
    for t in range(dmax):
        take_moments(t, t, mp_recv.at[t])
    blend(0, 0)
    for t in range(dmax):
        from_mate(t, 0, nb, past_recv.at[t])
        keep(t, t)
    for t in range(dmax):
        sent(t, 0, nb, past_send.at[t], pastf_send.at[t], past_recv.at[t])
        for copy in moment_copies(t, msend.at[t], mp_send.at[t], mp_recv.at[t]):
            copy.wait_send()
    small_in[3].wait()
    small_in[4].wait()
    for copy in tile_in:
        copy.wait()

    def current_of(n, b):
        pieces = []
        for j in range(near):
            ring = lax.rem(n + dmax - delay_ref[0, b, j], dmax)
            pieces.append(hist[ring * (WIN * nb) + pos[b * near + j]])
        gathered = jnp.concatenate(pieces, axis=1)
        field = jnp.dot(gathered, tiles[b].reshape(near * rows, rows), preferred_element_type=F32)
        far = jnp.dot(bl2[...], fin2[b], preferred_element_type=F32)
        driven = (inc[n, b].astype(F32) - field - far).astype(BF16)
        return jnp.dot(driven, sinv[b], preferred_element_type=F32).astype(BF16)

    def step(n, carry):
        t = n + dmax
        parity = n % 2
        later = (n + 1) % 2

        def sems(ch):
            return own_send.at[ch], fwd_send.at[ch], own_recv.at[parity, ch]

        def chunk(ch, moment):
            for i in range(per):
                b = ch * per + i
                value = current_of(n, b)
                win[t, own, b] = value
                out_ref[n, 0, b] = value
                moment = moment + jnp.dot(value, fout[b], preferred_element_type=F32)
            ssem, fsem, rsem = sems(ch)
            start(own_copies(t, ch, per, ssem, rsem))
            return moment

        moment = lax.fori_loop(0, chunks, chunk, jnp.zeros((pulses, rank), F32))
        msend[0] = pack(moment).astype(BF16)
        far_copies = moment_copies(t, msend.at[0], m_send, m_recv.at[parity])
        for copy in far_copies:
            copy.start()
        for hop in range(1, HOPS + 1):
            for ch in range(chunks):
                ssem, fsem, rsem = sems(ch)
                pass_on(t, ch, per, hop, fsem, rsem)
        ring = lax.rem(t, dmax)
        take_moments(t, ring, m_recv.at[parity])
        blend(n + 1, later)
        for ch in range(chunks):
            ssem, fsem, rsem = sems(ch)
            from_mate(t, ch, per, rsem)
        keep(t, ring)
        for ch in range(chunks):
            ssem, fsem, rsem = sems(ch)
            sent(t, ch, per, ssem, fsem, rsem)
        for copy in far_copies:
            copy.wait_send()
        return carry

    lax.fori_loop(0, steps - 1, step, 0)

    def last(b, carry):
        out_ref[steps - 1, 0, b] = current_of(steps - 1, b)
        return carry

    lax.fori_loop(0, nb, last, 0)


def on_device(
    regions, devices,
    incident, past_currents, self_inverse, near_tiles, near_cols, near_delay,
    block_slot, far_out, far_in, far_pairs, far_delay, far_coupling,
):
    steps, _, nb, pulses, rows = incident.shape
    dmax = past_currents.shape[0]
    near = near_cols.shape[2]
    rank = far_out.shape[3]
    farp = far_pairs.shape[1]
    places = devices // CORES
    half = pulses // 2
    chunks = 4
    times = dmax + steps - 1
    dma = pltpu.SemaphoreType.DMA
    smem = pl.BlockSpec(memory_space=pltpu.SMEM)
    anywhere = pl.BlockSpec(memory_space=pl.ANY)
    scratch = [
        pltpu.VMEM((times, WIN, nb, pulses, rows), BF16),
        pltpu.VMEM((dmax * WIN * nb, pulses, rows), BF16),
        pltpu.VMEM((nb, near, rows, rows), BF16),
        pltpu.VMEM((steps, nb, pulses, rows), BF16),
        pltpu.VMEM((nb, rows, rows), BF16),
        pltpu.VMEM((nb, rows, rank), BF16),
        pltpu.VMEM((nb, rank, rows), BF16),
        pltpu.VMEM((nb, 2 * rank, rows), BF16),
        pltpu.VMEM((farp, rank, rank), F32),
        pltpu.VMEM((farp, 2 * rank, 2 * rank), F32),
        pltpu.VMEM((dmax, half, 2 * rank), BF16),
        pltpu.VMEM((times, regions, places, half, 2 * rank), BF16),
        pltpu.VMEM((dmax, regions, half, 2 * rank), F32),
        pltpu.VMEM((half, 2 * rank), F32),
        pltpu.VMEM((2, half, 2 * rank), F32),
        pltpu.VMEM((pulses, 2 * rank), BF16),
        pltpu.SMEM((nb * near,), jnp.int32),
        dma((5,)),
        dma((dmax,)),
        dma((nb,)),
        dma((chunks, 3)),
        dma((chunks, HOPS, 2, 2)),
        dma((2, chunks, WIN)),
        dma((dmax, 3)),
        dma((dmax, HOPS, 2, 2)),
        dma((dmax, WIN)),
        dma((regions - 1, places)),
        dma((2, regions, places)),
        dma((dmax, regions - 1, places)),
        dma((dmax, regions, places)),
        dma,
        dma((2,)),
    ]
    return pl.pallas_call(
        functools.partial(march, regions, devices, chunks),
        out_shape=jax.ShapeDtypeStruct(incident.shape, BF16),
        in_specs=[smem] * 5 + [anywhere] * 7,
        out_specs=pl.BlockSpec(memory_space=pltpu.VMEM),
        scratch_shapes=scratch,
        compiler_params=pltpu.CompilerParams(
            collective_id=0, has_side_effects=True, vmem_limit_bytes=56 * 1024 * 1024
        ),
        name="march",
    )(
        near_cols, near_delay, block_slot, far_pairs, far_delay,
        incident, past_currents, self_inverse, near_tiles, far_out, far_in, far_coupling,
    )


def solution(mesh):
    in_specs = (
        P(None, "region", "blk", None, None),
        P(None, "region", "blk", None, None),
        P("region", "blk", None, None),
        P("region", "blk", None, None, None),
        P("region", "blk", None),
        P("region", "blk", None),
        P("region", None),
        P("region", "blk", None, None),
        P("region", "blk", None, None),
        P("region", None),
        P("region", None),
        P("region", None, None, None),
    )
    out_specs = P(None, "region", "blk", None, None)
    body = functools.partial(on_device, mesh.shape["region"], mesh.shape["blk"])
    return jax.shard_map(
        body, mesh=mesh, in_specs=in_specs, out_specs=out_specs, check_vma=False
    )
```
